32 devices in a mesh: gx: 4 (over y, core), gy: 8 (over z, x).
Axes of the slice: x: 2, y: 2, z: 4, core: 2. Of those that a mesh axis runs over, the one named last changes fastest.
Arguments:
- disp: float32 [3, 32, 128, 128], P(None, 'gx', 'gy'), may hold values from -3 to 3
- vel: float32 [3, 32, 128, 128], P(None, 'gx', 'gy'), may hold values from -30 to 30
- load: float32 [3, 32, 128, 128], P(None, 'gx', 'gy'), may hold values from -96 to 96
- flags: int32 [32, 128, 128], P('gx', 'gy'), may hold values 0 or 1
- mask_bits: int32 [4, 32, 128, 128], P(None, 'gx', 'gy'), may hold values from 0 to 2147483647, as said below
Outputs:
- disp_out: float32 [3, 32, 128, 128], P(None, 'gx', 'gy')
- vel_out: float32 [3, 32, 128, 128], P(None, 'gx', 'gy')
The draws below stay inside these ranges and needn't reach their ends.
Inputs may be any that keep to these rules, and one draw needn't show every extreme that they name: `mask_bits`: bit b (0 to 30) of word w marks the cell's bond to neighbour number 31 w + b as broken; bit 31, and bits of numbers 122 and above, are zero.
All inputs are finite; a program needn't handle non-finite values. No bound on the sum of `flags` on one device may be relied on, other than what follows from the above.
Results may differ from the reference program's by a relative error of at most 0.0001.
Values sent between devices are 32-bit elements; how exact they have to be, the bound alone decides.
No kernel may reach another device: no remote copies, remote signals or barrier semaphores. Data moves between devices by JAX's collectives and lax.ppermute only.
A program may use at most 128 MiB of HBM per device.

```python
import math
import jax
import jax.numpy as jnp
from jax import lax

NZ = 128
ITERS = 8
NX = 32
NY = 128


def neighbour_table_drawn():
    table = []
    for across in range(-3, 4):
        for along in range(-3, 4):
            for upward in range(-3, 4):
                length = across * across + along * along + upward * upward
                if 0 < length <= 9:
                    table.append((across, along, upward))
    return table


def draw_vel(key, part):
    places_x = jnp.arange(NX, dtype=jnp.float32) / max(NX - 1, 1)
    places_y = jnp.arange(NY, dtype=jnp.float32) / max(NY - 1, 1)
    amplitude = 0.3 * (1.0 + 2.0 * places_x)[:, None, None] * (1.0 + 2.0 * places_y)[None, :, None]
    first = jax.random.fold_in(key, 11)
    base = jnp.clip(jax.random.normal(first, (3, NX, NY, NZ), jnp.float32), -4.0, 4.0)
    return (amplitude[None] * base).astype(jnp.float32)


def draw_mask_bits(key, part):
    table = neighbour_table_drawn()
    places_x = jnp.arange(NX, dtype=jnp.int32)[:, None, None]
    places_y = jnp.arange(NY, dtype=jnp.int32)[None, :, None]
    middle = NX // 2
    words = []
    for word in range(4):
        packed = jnp.zeros((NX, NY, NZ), jnp.int32)
        for bit in range(31):
            number = 31 * word + bit
            if number < 122:
                across = table[number][0]
                coin = jax.random.randint(jax.random.fold_in(key, 100 + number), (NX, NY, NZ), 0, 16)
                crosses = (places_x < middle) & (places_x + across >= middle) | (places_x >= middle) & (places_x + across < middle)
                crack = crosses & (places_y < NY // 2)
                broken = (coin == 0) | crack
                packed = packed | broken.astype(jnp.int32) << bit
        words.append(packed)
    return jnp.stack(words)


def set_ends(array, rng, low, high):
    index_at = [jax.random.randint(jax.random.fold_in(rng, axis), (), 0, length) for axis, length in enumerate(array.shape)]
    widest = array.shape.index(max(array.shape))
    next_to = index_at[:widest] + [(index_at[widest] + 1) % array.shape[widest]] + index_at[widest + 1:]
    return array.at[tuple(index_at)].set(low).at[tuple(next_to)].set(high)


def level_of(rng, dims, split, low, high):
    factor_of = 1.0
    for dim, shards_of in split:
        steps = jax.random.uniform(jax.random.fold_in(jax.random.fold_in(rng, 6), dim), (shards_of,), jnp.float32, low / len(split), high / len(split))
        factor_of = factor_of * jnp.repeat(jnp.exp(steps), dims[dim] // shards_of).reshape((-1,) + (1,) * (len(dims) - 1 - dim))
    return factor_of


def scatter_about(own_key, dims, spread, bound, split=(), kind=jnp.bfloat16):
    factor_of = level_of(own_key, dims, split, -0.22, 0.18) if split else 1.0
    entries = jax.random.normal(own_key, dims, jnp.float32) * spread * factor_of
    return jnp.minimum(jnp.maximum(entries, -bound), bound).astype(kind)


def setup_inputs(seed: int = 0) -> dict:
    key_of = jax.random.split(jax.random.key(seed), 6)
    return {
        "disp": scatter_about(key_of[0], (3, NX, NY, NZ), 0.5, 3.0, ((1, 4), (2, 8)), jnp.float32),
        "vel": draw_vel(jax.random.fold_in(key_of[5], 71), 0),
        "load": scatter_about(key_of[2], (3, NX, NY, NZ), 16.0, 96.0, ((1, 4), (2, 8)), jnp.float32),
        "flags": set_ends((jax.random.randint(key_of[3], (NX, NY, NZ), 0, 3) < 1).astype(jnp.int32), jax.random.fold_in(key_of[3], 1), 0, 1),
        "mask_bits": draw_mask_bits(jax.random.fold_in(key_of[5], 71), 0),
    }


fictive_mass = 64.0
epsilon = 1e-06

def neighbour_table():
    table = []
    for across in range(-3, 4):
        for along in range(-3, 4):
            for upward in range(-3, 4):
                length = across * across + along * along + upward * upward
                if 0 < length <= 9:
                    table.append((across, along, upward))
    return table

def bond_forces(field_pad, words, words_pad, exist_pad):
    rows = words.shape[1]
    cols = words.shape[2]
    depth = words.shape[3]
    centre = field_pad[:, 3:3 + rows, 3:3 + cols, 3:3 + depth]
    totals = [jnp.zeros((rows, cols, depth), jnp.float32) for index in range(3)]
    for number, offset in enumerate(neighbour_table()):
        across, along, upward = offset
        word, bit = divmod(number, 31)
        mirror_word, mirror_bit = divmod(121 - number, 31)
        window = (slice(3 + across, 3 + across + rows), slice(3 + along, 3 + along + cols), slice(3 + upward, 3 + upward + depth))
        other = field_pad[(slice(None),) + window]
        own_flag = words[word] >> bit & 1
        far_flag = words_pad[mirror_word][window] >> mirror_bit & 1
        intact = (own_flag | far_flag == 0) & (exist_pad[window] > 0)
        length = float(across * across + along * along + upward * upward)
        weight = 1.0 / (length * math.sqrt(length))
        stretch = float(across) * (other[0] - centre[0]) + float(along) * (other[1] - centre[1]) + float(upward) * (other[2] - centre[2])
        scaled = jnp.where(intact, stretch * weight, jnp.float32(0.0))
        totals[0] = totals[0] + float(across) * scaled
        totals[1] = totals[1] + float(along) * scaled
        totals[2] = totals[2] + float(upward) * scaled
    return jnp.stack(totals)

def reference(disp, vel, load, flags, mask_bits):
    words_pad = jnp.pad(mask_bits, ((0, 0), (3, 3), (3, 3), (3, 3)))
    exist_pad = jnp.pad(jnp.ones(mask_bits.shape[1:], jnp.int32), 3)
    applied = flags.astype(jnp.float32)[None] * load
    count = 3.0 * NX * NY * NZ

    def internal(field):
        field_pad = jnp.pad(field, ((0, 0), (3, 3), (3, 3), (3, 3)))
        return bond_forces(field_pad, mask_bits, words_pad, exist_pad)
    previous = lax.fori_loop(0, 1, lambda index, carry: internal(disp - vel), jnp.zeros_like(disp))

    def relax(index, state):
        field, speed, before = state
        current = internal(field)
        total = current + applied
        kinetic = jnp.sum(speed * speed)
        rayleigh = jnp.sum(speed * (before - current))
        damping = 2.0 * jnp.sqrt(rayleigh / count / (fictive_mass * (kinetic / count + epsilon)))
        alpha = (2.0 - damping) / (2.0 + damping)
        beta = 2.0 / (fictive_mass * (2.0 + damping))
        speed = alpha * speed + beta * total
        return (field + speed, speed, current)
    field, speed, before = lax.fori_loop(0, ITERS, relax, (disp, vel, previous))
    return (field, speed)
```

```python
import math

import jax
import jax.numpy as jnp
from jax import lax
from jax.experimental import pallas as pl
from jax.experimental.pallas import tpu as pltpu
from jax.sharding import PartitionSpec as P

ITERS = 8
MASS = 64.0
EPS = 1e-06
LEAD = 8
VMEM = pltpu.CompilerParams(vmem_limit_bytes=48 * 1024 * 1024)


def neighbour_table():
    table = []
    for a in range(-3, 4):
        for b in range(-3, 4):
            for c in range(-3, 4):
                if 0 < a * a + b * b + c * c <= 9:
                    table.append((a, b, c))
    return table


TABLE = neighbour_table()
COLUMNS = [(a, b) for a in range(-3, 4) for b in range(-3, 4) if a * a + b * b <= 9]


def place(a, b, c):
    if abs(c) == 3:
        return 2 + (2 if c > 0 else -2), 29
    return 2 + c, COLUMNS.index((a, b))


def weight(a, b, c):
    length = float(a * a + b * b + c * c)
    return 1.0 / (length * math.sqrt(length) * MASS)


def shifted(x, axis, up):
    ends = lax.axis_size(axis) - 1
    if up:
        pairs = [(i, i + 1) for i in range(ends)]
    else:
        pairs = [(i + 1, i) for i in range(ends)]
    return lax.ppermute(x, axis, pairs)


def halos(q, outside=None):
    rows, cols = q.shape[1], q.shape[2]

    def edge(lo, hi, axis):
        if outside is None:
            return lo, hi
        at = lax.axis_index(axis)
        lo = jnp.where(at == 0, outside, lo)
        hi = jnp.where(at == lax.axis_size(axis) - 1, outside, hi)
        return lo, hi

    yl = shifted(q[:, :, cols - 3 :], "gy", True)
    yr = shifted(q[:, :, :3], "gy", False)
    yl, yr = edge(yl, yr, "gy")

    def strip(part):
        return jnp.concatenate([yl[:, part], q[:, part], yr[:, part]], axis=2)

    xl = shifted(strip(slice(rows - 3, rows)), "gx", True)
    xr = shifted(strip(slice(0, 3)), "gx", False)
    xl, xr = edge(xl, xr, "gx")
    return yl, yr, xl, xr


def fill(ext, q, yl, yr, xl, xr, shift):
    fields, rows, cols, depth = q.shape
    for f in range(fields):
        base = q[f, 0, 0:1, 0:1] if shift else None

        def moved(x):
            return x - base if shift else x

        ext[f, 3 : 3 + rows, LEAD : LEAD + cols, :] = moved(q[f])
        ext[f, 3 : 3 + rows, LEAD - 3 : LEAD, :] = moved(yl[f])
        ext[f, 3 : 3 + rows, LEAD + cols : LEAD + cols + 3, :] = moved(yr[f])
        ext[f, 0:3, LEAD - 3 : LEAD + cols + 3, :] = moved(xl[f])
        ext[f, 3 + rows :, LEAD - 3 : LEAD + cols + 3, :] = moved(xr[f])


def turn(x, by):
    depth = x.shape[-1]
    return pltpu.roll(x, by % depth, x.ndim - 1)


def prep_kernel(q, yl, yr, xl, xr, words_out, k_out, ext):
    _, rows, cols, depth = q.shape
    fill(ext, q, yl, yr, xl, xr, False)

    def row(r, carry):
        lane = lax.broadcasted_iota(jnp.int32, (8, depth), 1)
        for tile in range(cols // 8):
            at = pl.ds(tile * 8, 8)
            own = [q[w, r, at, :] for w in range(4)]
            bits = {c: jnp.zeros((8, depth), jnp.int32) for c in range(-3, 4)}
            ks = [jnp.zeros((8, depth), jnp.float32) for _ in range(6)]
            for number, (a, b, c) in enumerate(TABLE):
                word, bit = divmod(number, 31)
                mword, mbit = divmod(121 - number, 31)
                far = ext[mword, r + 3 + a, LEAD + tile * 8 + b : LEAD + tile * 8 + b + 8, :]
                if c:
                    far = turn(far, -c)
                broken = ((own[word] >> bit) | (far >> mbit)) & 1
                whole = broken == 0
                if c > 0:
                    whole = whole & (lane < depth - c)
                if c < 0:
                    whole = whole & (lane >= -c)
                slot = place(a, b, c)[1]
                bits[c] = bits[c] | jnp.where(whole, jnp.int32(1 << slot), 0)
                m = jnp.where(whole, jnp.float32(weight(a, b, c)), 0.0)
                for i, g in enumerate((a * a, b * b, c * c, a * b, a * c, b * c)):
                    if g:
                        ks[i] = ks[i] + (m if g == 1 else m * float(g))
            for c in range(-2, 3):
                value = turn(bits[c], c) if c else bits[c]
                if abs(c) == 2:
                    far = 3 if c > 0 else -3
                    value = value | turn(bits[far], far)
                words_out[2 + c, r, at, :] = value
            for i in range(6):
                k_out[i, r, at, :] = ks[i]
        return carry

    lax.fori_loop(0, rows, row, 0)


def plus(acc, x):
    return x if acc is None else acc + x


def forces(ext, words, k, r, tile, chains):
    at = pl.ds(tile * 8, 8)
    bits = [words[w, r, at, :] for w in range(5)]
    out = [[None, None, None] for _ in range(chains)]
    for group in ((0, 1, -1), (2, -2, 3, -3)):
        acc = {(ch, c): [None, None, None] for ch in range(chains) for c in group}
        for big in range(4):
            for wide in range(4):
                levels = [c for c in group if 0 < big * big + wide * wide + c * c <= 9]
                if not levels:
                    continue
                signs_a = (1, -1) if big else (1,)
                signs_b = (1, -1) if wide else (1,)
                t = {}
                for sa in signs_a:
                    for sb in signs_b:
                        a, b = sa * big, sb * wide
                        conds = {}
                        for c in levels:
                            w, bit = place(a, b, c)
                            conds[c] = (bits[w] & jnp.int32(1 << bit)) != 0
                        start = LEAD + tile * 8 + b
                        for ch in range(chains):
                            u = [
                                ext[3 * ch + i, r + 3 + a, start : start + 8, :]
                                for i in range(3)
                            ]
                            flat = None
                            if a:
                                flat = u[0] if a == 1 else u[0] * float(a)
                            if b:
                                side = u[1] if b == 1 else u[1] * float(b)
                                flat = side if flat is None else flat + side
                            for c in levels:
                                d = flat
                                if c:
                                    up = u[2] if abs(c) == 1 else u[2] * float(abs(c))
                                    if d is None:
                                        d = up if c > 0 else -up
                                    else:
                                        d = d + up if c > 0 else d - up
                                t[ch, c, sa, sb] = jnp.where(conds[c], d, 0.0)
                for ch in range(chains):
                    for c in levels:
                        w = weight(big, wide, c)
                        cell = acc[ch, c]
                        if big and wide:
                            p1 = t[ch, c, 1, 1] + t[ch, c, -1, 1]
                            q1 = t[ch, c, 1, 1] - t[ch, c, -1, 1]
                            p2 = t[ch, c, 1, -1] + t[ch, c, -1, -1]
                            q2 = t[ch, c, 1, -1] - t[ch, c, -1, -1]
                            total, dx, dy = p1 + p2, q1 + q2, p1 - p2
                        elif big:
                            total = t[ch, c, 1, 1] + t[ch, c, -1, 1]
                            dx, dy = t[ch, c, 1, 1] - t[ch, c, -1, 1], None
                        elif wide:
                            total = t[ch, c, 1, 1] + t[ch, c, 1, -1]
                            dx, dy = None, t[ch, c, 1, 1] - t[ch, c, 1, -1]
                        else:
                            total, dx, dy = t[ch, c, 1, 1], None, None
                        if dx is not None:
                            cell[0] = plus(cell[0], dx * (w * big))
                        if dy is not None:
                            cell[1] = plus(cell[1], dy * (w * wide))
                        if c:
                            cell[2] = plus(cell[2], total * (w * c))
        for ch in range(chains):
            for c in group:
                for i in range(3):
                    x = acc[ch, c][i]
                    if x is not None:
                        out[ch][i] = plus(out[ch][i], turn(x, -c) if c else x)
    for ch in range(chains):
        u = [ext[3 * ch + i, r + 3, LEAD + tile * 8 : LEAD + tile * 8 + 8, :] for i in range(3)]
        ks = [k[i, r, at, :] for i in range(6)]
        o = out[ch]
        o[0] = o[0] - (ks[0] * u[0] + ks[3] * u[1] + ks[4] * u[2])
        o[1] = o[1] - (ks[3] * u[0] + ks[1] * u[1] + ks[5] * u[2])
        o[2] = o[2] - (ks[4] * u[0] + ks[5] * u[1] + ks[2] * u[2])
    return out


def dot3(x, y):
    return x[0] * y[0] + x[1] * y[1] + x[2] * y[2]


def apply_kernel(kind, *refs):
    q, yl, yr, xl, xr, words, k = refs[:7]
    extra = refs[7:-3]
    q_out, sums, ext = refs[-3:]
    fields, rows, cols, depth = q.shape
    chains = fields // 3
    fill(ext, q, yl, yr, xl, xr, True)
    sums[...] = jnp.zeros_like(sums)

    def row(r, carry):
        for tile in range(cols // 8):
            at = pl.ds(tile * 8, 8)
            out = forces(ext, words, k, r, tile, chains)
            was = [[q[3 * ch + i, r, at, :] for i in range(3)] for ch in range(chains)]
            if kind == "first":
                load, flags = extra
                on = flags[r, at, :].astype(jnp.float32) * (1.0 / MASS)
                for i in range(3):
                    out[0][i] = out[0][i] + on * load[i, r, at, :]
            for ch in range(chains):
                for i in range(3):
                    q_out[3 * ch + i, r, at, :] = out[ch][i]
            y_old, y_new = was[0], out[0]
            if kind == "last":
                x_old = [extra[0][3 + i, r, at, :] for i in range(3)]
            else:
                x_old, x_new = was[1], out[1]
                sums[0] += dot3(x_old, x_old)
                sums[1] += dot3(x_old, x_new)
            if kind != "last":
                sums[3] += dot3(x_old, y_new)
            if kind != "first":
                sums[2] += dot3(x_old, y_old)
                sums[4] += dot3(y_old, y_old)
                sums[5] += dot3(y_old, y_new)
        return carry

    lax.fori_loop(0, rows, row, 0)


def hankel(p, q, moments, lift):
    a, b, c = moments
    total = None
    n = len(p)
    for order in range(2 * n - 1):
        pp = pq = qq = None
        for i in range(n):
            j = order - i
            if not 0 <= j < n:
                continue
            if p[i] is not None and p[j] is not None and i <= j:
                z = p[i] * p[j]
                pp = plus(pp, z + z if i < j else z)
            if q[i] is not None and q[j] is not None and i <= j:
                z = q[i] * q[j]
                qq = plus(qq, z + z if i < j else z)
            if p[i] is not None and q[j] is not None:
                z = p[i] * q[j]
                pq = plus(pq, z + z)
        for mine, table in ((pp, a), (pq, b), (qq, c)):
            if mine is not None:
                total = plus(total, mine * table[order + lift])
    return total


def added(x, y):
    if x is None:
        return y
    return x if y is None else x + y


def finish_kernel(count, rounds, *refs):
    m, disp, vel = refs[:3]
    qs = refs[3 : 3 + rounds]
    u_out, v_out = refs[-2:]
    rows, cols, depth = disp.shape[1:]

    def moment(step, which):
        at = 6 * step + which
        return m[at : at + 1, :]

    a, b, c = {}, {}, {}
    for s in range(rounds):
        a[2 * s], a[2 * s + 1] = moment(s, 0), moment(s, 1)
        b[2 * s] = moment(s, 3)
        if s:
            b[2 * s - 1] = moment(s, 2)
            c[2 * s - 2], c[2 * s - 1] = moment(s, 4), moment(s, 5)
    one = jnp.ones((1, depth), jnp.float32)
    p, q = [one], [None]
    r, t = [None], [one]
    up, uq = [None] * rounds, [None] * rounds
    for step in range(rounds):
        kinetic = hankel(p, q, (a, b, c), 0) * (1.0 / count)
        rayleigh = jnp.maximum(-hankel(p, q, (a, b, c), 1), 0.0) * (1.0 / count)
        damping = 2.0 * jnp.sqrt(rayleigh / (kinetic + EPS))
        beta = 2.0 / (2.0 + damping)
        alpha = (2.0 - damping) / (2.0 + damping)

        def mixed(own, other):
            own = own + [None] * (len(other) - len(own))
            return [
                added(
                    None if x is None else alpha * x, None if y is None else beta * y
                )
                for x, y in zip(own, other)
            ]

        p, q = mixed(p, r), mixed(q, t)
        for j in range(len(p)):
            up[j], uq[j] = added(up[j], p[j]), added(uq[j], q[j])
        r = [added(x, y) for x, y in zip(r + [None], [None] + p)]
        t = [added(x, y) for x, y in zip(t + [None], [None] + q)]
    p, q = p[:rounds], q[:rounds]

    def row(at_row, carry):
        for tile in range(cols // 8):
            at = pl.ds(tile * 8, 8)
            for i in range(3):
                u, v = disp[i, at_row, at, :], None
                for j in range(rounds):
                    x = vel[i, at_row, at, :] if j == 0 else qs[j - 1][3 + i, at_row, at, :]
                    y = qs[j][i, at_row, at, :]
                    u = u + up[j] * x + uq[j] * y
                    v = plus(v, p[j] * x + q[j] * y)
                u_out[i, at_row, at, :] = u
                v_out[i, at_row, at, :] = v
        return carry

    lax.fori_loop(0, rows, row, 0)


def summed(x):
    for axis in ("gx", "gy"):
        size = lax.axis_size(axis)
        if size & (size - 1):
            x = lax.psum(x, axis)
            continue
        step = 1
        while step < size:
            x = x + lax.ppermute(x, axis, [(i, i ^ step) for i in range(size)])
            step *= 2
    return x


def on_device(disp, vel, load, flags, mask_bits):
    _, rows, cols, depth = disp.shape
    count = 3.0 * rows * lax.axis_size("gx") * cols * lax.axis_size("gy") * depth
    f32, i32 = jnp.float32, jnp.int32

    def scratch(fields, kind):
        return [pltpu.VMEM((fields, rows + 6, cols + 2 * LEAD, depth), kind)]

    words, k = pl.pallas_call(
        prep_kernel,
        out_shape=(
            jax.ShapeDtypeStruct((5, rows, cols, depth), i32),
            jax.ShapeDtypeStruct((6, rows, cols, depth), f32),
        ),
        scratch_shapes=scratch(4, i32),
        compiler_params=VMEM,
        name="prep",
    )(mask_bits, *halos(mask_bits, -1))

    def applied_to(q, kind, *extra):
        fields = q.shape[0]

        def body(*refs):
            apply_kernel(kind, *refs)

        return pl.pallas_call(
            body,
            out_shape=(
                jax.ShapeDtypeStruct(q.shape, f32),
                jax.ShapeDtypeStruct((6, 8, depth), f32),
            ),
            scratch_shapes=scratch(fields, f32),
            compiler_params=VMEM,
            name="apply_" + kind,
        )(q, *halos(q), words, k, *extra)

    q, sums = applied_to(jnp.concatenate([disp, vel]), "first", load, flags)
    qs, parts = [q], [sums]
    for step in range(1, ITERS - 1):
        q, sums = applied_to(q, "mid")
        qs.append(q)
        parts.append(sums)
    last, sums = applied_to(q[:3], "last", q)
    qs.append(last)
    parts.append(sums)
    local = jnp.sum(jnp.stack(parts).reshape(6 * ITERS, 8 * depth), axis=1)
    moments = summed(jnp.pad(local, (0, 128 - 6 * ITERS)).reshape(1, 128))
    spread = jnp.broadcast_to(moments.reshape(128, 1)[: 6 * ITERS], (6 * ITERS, depth))

    def body(*refs):
        finish_kernel(count, ITERS, *refs)

    return pl.pallas_call(
        body,
        out_shape=(jax.ShapeDtypeStruct(disp.shape, f32), jax.ShapeDtypeStruct(vel.shape, f32)),
        compiler_params=VMEM,
        name="finish",
    )(spread, disp, vel, *qs)


def solution(mesh):
    placed = (
        P(None, "gx", "gy", None),
        P(None, "gx", "gy", None),
        P(None, "gx", "gy", None),
        P("gx", "gy", None),
        P(None, "gx", "gy", None),
    )
    return jax.shard_map(
        on_device,
        mesh=mesh,
        in_specs=placed,
        out_specs=(P(None, "gx", "gy", None), P(None, "gx", "gy", None)),
        check_vma=False,
    )
```

```python
import math

import jax
import jax.numpy as jnp
from jax import lax
from jax.experimental import pallas as pl
from jax.experimental.pallas import tpu as pltpu
from jax.sharding import PartitionSpec as P

ITERS = 8
MASS = 64.0
EPS = 1e-06
LEAD = 8
VMEM = pltpu.CompilerParams(vmem_limit_bytes=48 * 1024 * 1024)


def neighbour_table():
    table = []
    for a in range(-3, 4):
        for b in range(-3, 4):
            for c in range(-3, 4):
                if 0 < a * a + b * b + c * c <= 9:
                    table.append((b, a, c))
    return table


TABLE = neighbour_table()
COLUMNS = [(a, b) for a in range(-3, 4) for b in range(-3, 4) if a * a + b * b <= 9]


def place(a, b, c):
    if abs(c) == 3:
        return 2 + (2 if c > 0 else -2), 29
    return 2 + c, COLUMNS.index((a, b))


def weight(a, b, c):
    length = float(a * a + b * b + c * c)
    return 1.0 / (length * math.sqrt(length) * MASS)


def halos(q, outside=None):
    rows = q.shape[1]
    across, along = lax.axis_size("gx"), lax.axis_size("gy")
    slabs = [x * along + y for y in range(along) for x in range(across)]
    at = lax.axis_index("gy") * across + lax.axis_index("gx")
    lo, hi = [], []
    hops = -(-3 // rows)
    for hop in range(1, hops + 1):
        need = min(rows, 3 - (hop - 1) * rows)
        up = list(zip(slabs[:-hop], slabs[hop:]))
        below = lax.ppermute(q[:, rows - need :], ("gx", "gy"), up)
        above = lax.ppermute(q[:, :need], ("gx", "gy"), [(b, a) for a, b in up])
        if outside is not None:
            below = jnp.where(at < hop, outside, below)
            above = jnp.where(at >= len(slabs) - hop, outside, above)
        lo.insert(0, below)
        hi.append(above)
    if hops == 1:
        return lo[0], hi[0]
    return jnp.concatenate(lo, axis=1), jnp.concatenate(hi, axis=1)


def to_slabs(x):
    return lax.all_to_all(jnp.swapaxes(x, 1, 2), "gx", 1, 2, tiled=True)


def from_slabs(x):
    return jnp.swapaxes(lax.all_to_all(x, "gx", 2, 1, tiled=True), 1, 2)


def fill(ext, q, lo, hi, shift):
    fields, rows, cols, depth = q.shape
    for f in range(fields):
        base = q[f, 0, 0:1, 0:1] if shift else None

        def moved(x):
            return x - base if shift else x

        ext[f, 3 : 3 + rows, LEAD : LEAD + cols, :] = moved(q[f])
        ext[f, 0:3, LEAD : LEAD + cols, :] = moved(lo[f])
        ext[f, 3 + rows :, LEAD : LEAD + cols, :] = moved(hi[f])


def turn(x, by):
    depth = x.shape[-1]
    return pltpu.roll(x, by % depth, x.ndim - 1)


def prep_kernel(q, lo, hi, words_out, k_out, ext):
    _, rows, cols, depth = q.shape
    ext[...] = jnp.full_like(ext, -1)
    fill(ext, q, lo, hi, False)

    def row(r, carry):
        lane = lax.broadcasted_iota(jnp.int32, (8, depth), 1)
        for tile in range(cols // 8):
            at = pl.ds(tile * 8, 8)
            own = [q[w, r, at, :] for w in range(4)]
            bits = {c: jnp.zeros((8, depth), jnp.int32) for c in range(-3, 4)}
            ks = [jnp.zeros((8, depth), jnp.float32) for _ in range(6)]
            for number, (a, b, c) in enumerate(TABLE):
                word, bit = divmod(number, 31)
                mword, mbit = divmod(121 - number, 31)
                far = ext[mword, r + 3 + a, LEAD + tile * 8 + b : LEAD + tile * 8 + b + 8, :]
                if c:
                    far = turn(far, -c)
                broken = ((own[word] >> bit) | (far >> mbit)) & 1
                whole = broken == 0
                if c > 0:
                    whole = whole & (lane < depth - c)
                if c < 0:
                    whole = whole & (lane >= -c)
                slot = place(a, b, c)[1]
                bits[c] = bits[c] | jnp.where(whole, jnp.int32(1 << slot), 0)
                m = jnp.where(whole, jnp.float32(weight(a, b, c)), 0.0)
                for i, g in enumerate((a * a, b * b, c * c, a * b, a * c, b * c)):
                    if g:
                        ks[i] = ks[i] + (m if g == 1 else m * float(g))
            for c in range(-2, 3):
                value = turn(bits[c], c) if c else bits[c]
                if abs(c) == 2:
                    far = 3 if c > 0 else -3
                    value = value | turn(bits[far], far)
                words_out[2 + c, r, at, :] = value
            for i in range(6):
                k_out[i, r, at, :] = ks[i]
        return carry

    lax.fori_loop(0, rows, row, 0)


def plus(acc, x):
    return x if acc is None else acc + x


def forces(ext, words, k, r, tile, chains):
    at = pl.ds(tile * 8, 8)
    bits = [words[w, r, at, :] for w in range(5)]
    out = [[None, None, None] for _ in range(chains)]
    for group in ((0, 1, -1), (2, -2, 3, -3)):
        acc = {(ch, c): [None, None, None] for ch in range(chains) for c in group}
        for big in range(4):
            for wide in range(4):
                levels = [c for c in group if 0 < big * big + wide * wide + c * c <= 9]
                if not levels:
                    continue
                signs_a = (1, -1) if big else (1,)
                signs_b = (1, -1) if wide else (1,)
                t = {}
                for sa in signs_a:
                    for sb in signs_b:
                        a, b = sa * big, sb * wide
                        conds = {}
                        for c in levels:
                            w, bit = place(a, b, c)
                            conds[c] = (bits[w] & jnp.int32(1 << bit)) != 0
                        start = LEAD + tile * 8 + b
                        for ch in range(chains):
                            u = [
                                ext[3 * ch + i, r + 3 + a, start : start + 8, :]
                                for i in range(3)
                            ]
                            flat = None
                            if a:
                                flat = u[0] if a == 1 else u[0] * float(a)
                            if b:
                                side = u[1] if b == 1 else u[1] * float(b)
                                flat = side if flat is None else flat + side
                            for c in levels:
                                d = flat
                                if c:
                                    up = u[2] if abs(c) == 1 else u[2] * float(abs(c))
                                    if d is None:
                                        d = up if c > 0 else -up
                                    else:
                                        d = d + up if c > 0 else d - up
                                t[ch, c, sa, sb] = jnp.where(conds[c], d, 0.0)
                for ch in range(chains):
                    for c in levels:
                        w = weight(big, wide, c)
                        cell = acc[ch, c]
                        if big and wide:
                            p1 = t[ch, c, 1, 1] + t[ch, c, -1, 1]
                            q1 = t[ch, c, 1, 1] - t[ch, c, -1, 1]
                            p2 = t[ch, c, 1, -1] + t[ch, c, -1, -1]
                            q2 = t[ch, c, 1, -1] - t[ch, c, -1, -1]
                            total, dx, dy = p1 + p2, q1 + q2, p1 - p2
                        elif big:
                            total = t[ch, c, 1, 1] + t[ch, c, -1, 1]
                            dx, dy = t[ch, c, 1, 1] - t[ch, c, -1, 1], None
                        elif wide:
                            total = t[ch, c, 1, 1] + t[ch, c, 1, -1]
                            dx, dy = None, t[ch, c, 1, 1] - t[ch, c, 1, -1]
                        else:
                            total, dx, dy = t[ch, c, 1, 1], None, None
                        if dx is not None:
                            cell[0] = plus(cell[0], dx * (w * big))
                        if dy is not None:
                            cell[1] = plus(cell[1], dy * (w * wide))
                        if c:
                            cell[2] = plus(cell[2], total * (w * c))
        for ch in range(chains):
            for c in group:
                for i in range(3):
                    x = acc[ch, c][i]
                    if x is not None:
                        out[ch][i] = plus(out[ch][i], turn(x, -c) if c else x)
    for ch in range(chains):
        u = [ext[3 * ch + i, r + 3, LEAD + tile * 8 : LEAD + tile * 8 + 8, :] for i in range(3)]
        ks = [k[i, r, at, :] for i in range(6)]
        o = out[ch]
        o[0] = o[0] - (ks[0] * u[0] + ks[3] * u[1] + ks[4] * u[2])
        o[1] = o[1] - (ks[3] * u[0] + ks[1] * u[1] + ks[5] * u[2])
        o[2] = o[2] - (ks[4] * u[0] + ks[5] * u[1] + ks[2] * u[2])
    return out


def dot3(x, y):
    return x[0] * y[0] + x[1] * y[1] + x[2] * y[2]


def apply_kernel(kind, *refs):
    q, lo, hi, words, k = refs[:5]
    extra = refs[5:-3]
    q_out, sums, ext = refs[-3:]
    fields, rows, cols, depth = q.shape
    chains = fields // 3
    fill(ext, q, lo, hi, True)
    sums[...] = jnp.zeros_like(sums)

    def row(r, carry):
        for tile in range(cols // 8):
            at = pl.ds(tile * 8, 8)
            out = forces(ext, words, k, r, tile, chains)
            was = [[q[3 * ch + i, r, at, :] for i in range(3)] for ch in range(chains)]
            if kind == "first":
                for i in range(3):
                    out[0][i] = out[0][i] + extra[0][i, r, at, :] * (1.0 / MASS)
            for ch in range(chains):
                for i in range(3):
                    q_out[3 * ch + i, r, at, :] = out[ch][i]
            y_old, y_new = was[0], out[0]
            if kind == "last":
                x_old = [extra[0][3 + i, r, at, :] for i in range(3)]
            else:
                x_old, x_new = was[1], out[1]
                sums[0] += dot3(x_old, x_old)
                sums[1] += dot3(x_old, x_new)
            if kind != "last":
                sums[3] += dot3(x_old, y_new)
            if kind != "first":
                sums[2] += dot3(x_old, y_old)
                sums[4] += dot3(y_old, y_old)
                sums[5] += dot3(y_old, y_new)
        return carry

    lax.fori_loop(0, rows, row, 0)


def hankel(p, q, moments, lift):
    a, b, c = moments
    total = None
    n = len(p)
    for order in range(2 * n - 1):
        pp = pq = qq = None
        for i in range(n):
            j = order - i
            if not 0 <= j < n:
                continue
            if p[i] is not None and p[j] is not None and i <= j:
                z = p[i] * p[j]
                pp = plus(pp, z + z if i < j else z)
            if q[i] is not None and q[j] is not None and i <= j:
                z = q[i] * q[j]
                qq = plus(qq, z + z if i < j else z)
            if p[i] is not None and q[j] is not None:
                z = p[i] * q[j]
                pq = plus(pq, z + z)
        for mine, table in ((pp, a), (pq, b), (qq, c)):
            if mine is not None:
                total = plus(total, mine * table[order + lift])
    return total


def added(x, y):
    if x is None:
        return y
    return x if y is None else x + y


def finish_kernel(count, rounds, *refs):
    m, start = refs[:2]
    qs = refs[2 : 2 + rounds]
    out = refs[-1]
    rows, cols, depth = start.shape[1:]

    def moment(step, which):
        at = 6 * step + which
        return m[at : at + 1, :]

    a, b, c = {}, {}, {}
    for s in range(rounds):
        a[2 * s], a[2 * s + 1] = moment(s, 0), moment(s, 1)
        b[2 * s] = moment(s, 3)
        if s:
            b[2 * s - 1] = moment(s, 2)
            c[2 * s - 2], c[2 * s - 1] = moment(s, 4), moment(s, 5)
    one = jnp.ones((1, depth), jnp.float32)
    p, q = [one], [None]
    r, t = [None], [one]
    up, uq = [None] * rounds, [None] * rounds
    for step in range(rounds):
        kinetic = hankel(p, q, (a, b, c), 0) * (1.0 / count)
        rayleigh = jnp.maximum(-hankel(p, q, (a, b, c), 1), 0.0) * (1.0 / count)
        damping = 2.0 * jnp.sqrt(rayleigh / (kinetic + EPS))
        beta = 2.0 / (2.0 + damping)
        alpha = (2.0 - damping) / (2.0 + damping)

        def mixed(own, other):
            own = own + [None] * (len(other) - len(own))
            return [
                added(
                    None if x is None else alpha * x, None if y is None else beta * y
                )
                for x, y in zip(own, other)
            ]

        p, q = mixed(p, r), mixed(q, t)
        for j in range(len(p)):
            up[j], uq[j] = added(up[j], p[j]), added(uq[j], q[j])
        r = [added(x, y) for x, y in zip(r + [None], [None] + p)]
        t = [added(x, y) for x, y in zip(t + [None], [None] + q)]
    p, q = p[:rounds], q[:rounds]

    def row(at_row, carry):
        for tile in range(cols // 8):
            at = pl.ds(tile * 8, 8)
            for i in range(3):
                u, v = start[i, at_row, at, :], None
                for j in range(rounds):
                    x = start[3 + i, at_row, at, :] if j == 0 else qs[j - 1][3 + i, at_row, at, :]
                    y = qs[j][i, at_row, at, :]
                    u = u + up[j] * x + uq[j] * y
                    v = plus(v, p[j] * x + q[j] * y)
                out[i, at_row, at, :] = u
                out[3 + i, at_row, at, :] = v
        return carry

    lax.fori_loop(0, rows, row, 0)


def summed(x):
    for axis in ("gx", "gy"):
        size = lax.axis_size(axis)
        if size & (size - 1):
            x = lax.psum(x, axis)
            continue
        step = 1
        while step < size:
            x = x + lax.ppermute(x, axis, [(i, i ^ step) for i in range(size)])
            step *= 2
    return x


def on_device(disp, vel, load, flags, mask_bits):
    _, rows, cols, depth = disp.shape
    count = 3.0 * rows * lax.axis_size("gx") * cols * lax.axis_size("gy") * depth
    f32, i32 = jnp.float32, jnp.int32
    applied = flags.astype(f32)[None] * load
    parts = [x[i : i + 1] for x in (disp, vel, applied) for i in (1, 0, 2)]
    fields = to_slabs(jnp.concatenate(parts))
    masks = to_slabs(mask_bits)
    start, applied = fields[:6], fields[6:]
    _, rows, cols, depth = start.shape

    def scratch(fields, kind):
        return [pltpu.VMEM((fields, rows + 6, cols + 2 * LEAD, depth), kind)]

    words, k = pl.pallas_call(
        prep_kernel,
        out_shape=(
            jax.ShapeDtypeStruct((5, rows, cols, depth), i32),
            jax.ShapeDtypeStruct((6, rows, cols, depth), f32),
        ),
        scratch_shapes=scratch(4, i32),
        compiler_params=VMEM,
        name="prep",
    )(masks, *halos(masks, -1))

    def applied_to(q, kind, *extra):
        fields = q.shape[0]

        def body(*refs):
            apply_kernel(kind, *refs)

        return pl.pallas_call(
            body,
            out_shape=(
                jax.ShapeDtypeStruct(q.shape, f32),
                jax.ShapeDtypeStruct((6, 8, depth), f32),
            ),
            scratch_shapes=scratch(fields, f32),
            compiler_params=VMEM,
            name="apply_" + kind,
        )(q, *halos(q), words, k, *extra)

    q, sums = applied_to(start, "first", applied)
    qs, parts = [q], [sums]
    for step in range(1, ITERS - 1):
        q, sums = applied_to(q, "mid")
        qs.append(q)
        parts.append(sums)
    last, sums = applied_to(q[:3], "last", q)
    qs.append(last)
    parts.append(sums)
    local = jnp.sum(jnp.stack(parts).reshape(6 * ITERS, 8 * depth), axis=1)
    moments = summed(jnp.pad(local, (0, 128 - 6 * ITERS)).reshape(1, 128))
    spread = jnp.broadcast_to(moments.reshape(128, 1)[: 6 * ITERS], (6 * ITERS, depth))

    def body(*refs):
        finish_kernel(count, ITERS, *refs)

    done = pl.pallas_call(
        body,
        out_shape=jax.ShapeDtypeStruct(start.shape, f32),
        compiler_params=VMEM,
        name="finish",
    )(spread, start, *qs)
    done = from_slabs(done)
    u, v = ([done[base + i] for i in (1, 0, 2)] for base in (0, 3))
    return jnp.stack(u), jnp.stack(v)


def solution(mesh):
    placed = (
        P(None, "gx", "gy", None),
        P(None, "gx", "gy", None),
        P(None, "gx", "gy", None),
        P("gx", "gy", None),
        P(None, "gx", "gy", None),
    )
    return jax.shard_map(
        on_device,
        mesh=mesh,
        in_specs=placed,
        out_specs=(P(None, "gx", "gy", None), P(None, "gx", "gy", None)),
        check_vma=False,
    )
```
